32 devices in a mesh: dp: 8 (over z, core), expert: 4 (over y, x).
Axes of the slice: x: 2, y: 2, z: 4, core: 2. Of those that a mesh axis runs over, the one named last changes fastest.
Arguments:
- tokens: bfloat16 [4096, 4096], P(('dp', 'expert')), may hold values from -6 to 6
- norm_gain: float32 [4096], replicated, may hold values from 0.5 to 1.5
- recorded_ids: int32 [32, 128, 8], P(None, ('dp', 'expert')), may hold values from 0 to 31, all different within a row; in each aligned block of 128 rows (0 to 127, 128 to 255, ..., all dimensions but the last counted through in order) at most 48 rows name the same one
- recorded_gates: float32 [32, 128, 8], P(None, ('dp', 'expert')), may hold values from 0.05 to 1
- w_gate: bfloat16 [32, 4096, 768], P(('dp', 'expert')), may hold values from -0.09375 to 0.09375
- w_up: bfloat16 [32, 4096, 768], P(('dp', 'expert')), may hold values from -0.09375 to 0.09375
- w_down: bfloat16 [32, 768, 4096], P(('dp', 'expert')), may hold values from -0.21875 to 0.21875
Outputs:
- combined: bfloat16 [4096, 4096], P(('dp', 'expert'))
The draws below stay inside these ranges and needn't reach their ends.
Inputs may be any that keep to these rules, and one draw needn't show every extreme that they name: `recorded_ids`: each token names 8 different experts. Among the 128 tokens of one sequence no expert is named by more than 48 tokens, a bound that some block reaches.
All inputs are finite; a program needn't handle non-finite values.
Results may differ from the reference program's by a relative error of at most 0.0071.
Values may be sent and summed in bfloat16 or wider, within the bound.
No kernel may reach another device: no remote copies, remote signals or barrier semaphores. Data moves between devices by JAX's collectives and lax.ppermute only.
A program may use at most 128 MiB of HBM per device.

```python
import math
import jax
import jax.numpy as jnp
import numpy as np
from jax import lax

D = 4096
FF = 768
TOP = 8
LENGTH = 128
SEQS = 32
EXPERTS = 32
TOKENS = 4096
MOST = 48
CAP = 1280


def shard_levels(stream_key, shape, pieces, low, top_value):
    factor_of = 1.0
    for dim, parts in pieces:
        draws = jax.random.uniform(jax.random.fold_in(jax.random.fold_in(stream_key, 6), dim), (parts,), jnp.float32, low / len(pieces), top_value / len(pieces))
        factor_of = factor_of * jnp.repeat(jnp.exp(draws), shape[dim] // parts).reshape((-1,) + (1,) * (len(shape) - 1 - dim))
    return factor_of


def routed_block(stream_key, own, number, rows, count, top, most, lean):
    sequence = jax.random.permutation(stream_key, count)
    packed, common = load_shares(count, rows * top, most, lean, True), load_shares(count, rows * top, most, lean, False)
    places = jnp.arange(count)

    def named(tallies, turn):
        used = int((tallies > 0).sum())
        fixed = max(1, used // 4)
        moved = fixed + (places - fixed + turn * (used - fixed)) % max(1, count - fixed)
        return jnp.zeros((count,), jnp.int32).at[sequence[jnp.where(places < fixed, places, moved)]].set(jnp.asarray(tallies, jnp.int32))

    tallies = jnp.where(number % 4 == 0, named(packed, number // 4), named(common, number - number // 4 - 1))
    mixed = jax.random.permutation(jax.random.fold_in(own, 3), count)
    source_of, receiver = mixed[0:count // 2 * 2:2], mixed[1:count // 2 * 2:2]
    margin = jnp.minimum(tallies[source_of] - 1, most - tallies[receiver]) // 2
    margin = jnp.where((source_of == sequence[0]) | (receiver == sequence[0]) | (tallies[receiver] == 0), 0, jnp.maximum(margin, 0))
    moved = jax.random.randint(jax.random.fold_in(own, 4), (count // 2,), 0, 1 << 20) % (margin + 1)
    tallies = tallies.at[source_of].add(-moved).at[receiver].add(moved)
    members = jnp.searchsorted(jnp.cumsum(tallies), jnp.arange(rows * top), side="right").astype(jnp.int32)
    table = members.reshape(top, rows).T
    table = table[jax.random.permutation(jax.random.fold_in(own, 1), rows)]
    turn = jax.random.randint(jax.random.fold_in(own, 2), (rows, 1), 0, top)
    return jnp.take_along_axis(table, (jnp.arange(top)[None, :] + turn) % top, axis=1)


def load_shares(count, total, limit, lean, full):
    portions = [(1 << 20) // math.isqrt(grade ** lean) + 1 for grade in range(1, count + 1)]
    largest = limit if full else min(limit, max(-(-total // count), total * portions[0] // sum(portions)))
    least = 1 if total - largest >= count - 1 else 0
    given, rest = [largest] + [least] * (count - 1), total - largest - least * (count - 1)
    while rest > 0:
        movable = [i for i in range(1, count) if given[i] < largest] or [i for i in range(1, count) if given[i] < limit]
        pool, remaining = sum([portions[i] for i in movable]), rest
        for i in movable:
            more = min(limit - given[i], max(1, remaining * portions[i] // pool), rest)
            given[i] = given[i] + more
            rest = rest - more
    return np.array(given)


def noise(rng, extent, width, bound, cuts=(), kind=jnp.bfloat16):
    array = jax.random.normal(rng, extent, jnp.float32) * width
    if len(cuts) > 0:
        array = shard_levels(rng, extent, cuts, -0.22, 0.18) * array
    return jnp.clip(array, min=-bound, max=bound).astype(kind)


def setup_inputs(seed: int = 0) -> dict:
    streams_of = jax.random.split(jax.random.key(seed), 8)
    tokens = noise(streams_of[0], (TOKENS, D), 1.0, 6.0, ((0, 32),))
    norm_gain = jnp.clip(1.0 + 0.1 * jax.random.normal(streams_of[1], (D,), jnp.float32), 0.5, 1.5)
    recorded_ids_keys = jax.random.split(jax.random.fold_in(streams_of[2], 1), SEQS * LENGTH // LENGTH)
    recorded_ids_turns = jax.random.permutation(jax.random.fold_in(streams_of[2], 3), SEQS * LENGTH // LENGTH)
    recorded_ids = jax.vmap(lambda own, number: routed_block(jax.random.fold_in(streams_of[2], 2), own, number, LENGTH, EXPERTS, TOP, MOST, 2))(recorded_ids_keys, recorded_ids_turns).reshape((SEQS, LENGTH, TOP))
    recorded_gates = jnp.clip(jnp.exp(math.log(1.0) - 2.9957323 * jax.random.uniform(streams_of[3], (SEQS, LENGTH, TOP), jnp.float32) ** shard_levels(streams_of[3], (SEQS, LENGTH, TOP), ((1, 32),), -0.2, 0.2)), 0.05, 1.0)
    w_gate = noise(streams_of[4], (EXPERTS, D, FF), D ** -0.5, 0.09375, ((0, 32),))
    w_up = noise(streams_of[5], (EXPERTS, D, FF), D ** -0.5, 0.09375, ((0, 32),))
    w_down = noise(streams_of[6], (EXPERTS, FF, D), FF ** -0.5, 0.21875, ((0, 32),))
    return dict(tokens=tokens, norm_gain=norm_gain, recorded_ids=recorded_ids, recorded_gates=recorded_gates, w_gate=w_gate, w_up=w_up, w_down=w_down)


EPSILON = 1e-06

def rms_normed(tokens, norm_gain):
    widened = tokens.astype(jnp.float32)
    spread = lax.optimization_barrier(jnp.mean(widened * widened, axis=-1, keepdims=True))
    return (widened * lax.rsqrt(spread + EPSILON) * norm_gain.astype(jnp.float32)).astype(jnp.bfloat16)

def reference(tokens, norm_gain, recorded_ids, recorded_gates, w_gate, w_up, w_down):
    normed = rms_normed(tokens, norm_gain)
    route_ids = recorded_ids.reshape(-1).astype(jnp.int32)
    route_gates = recorded_gates.reshape(-1)
    assignments = route_ids.shape[0]
    onehot = (route_ids[:, None] == jnp.arange(EXPERTS, dtype=jnp.int32)[None, :]).astype(jnp.int32)
    before = jnp.cumsum(onehot, axis=0) - onehot
    position = lax.optimization_barrier(jnp.sum(before * onehot, axis=1)).astype(jnp.int32)
    token_of = (jnp.arange(assignments, dtype=jnp.int32) // TOP).astype(jnp.int32)

    def one_expert(running, inputs):
        gate_matrix, up_matrix, down_matrix, expert = inputs
        chosen = (route_ids == expert) & (position < CAP)
        target = jnp.where(chosen, position, CAP).astype(jnp.int32)
        owner_token = jnp.zeros((CAP + 1,), jnp.int32).at[target].set(token_of)[:CAP]
        filled = jnp.zeros((CAP + 1,), jnp.bool_).at[target].set(chosen)[:CAP]
        weight_slot = jnp.zeros((CAP + 1,), jnp.float32).at[target].set(route_gates)[:CAP]
        gathered = jnp.where(filled[:, None], normed[owner_token], jnp.zeros((), jnp.bfloat16))
        gate_part = jnp.dot(gathered, gate_matrix, preferred_element_type=jnp.float32)
        up_part = jnp.dot(gathered, up_matrix, preferred_element_type=jnp.float32)
        hidden = (jax.nn.silu(gate_part) * up_part).astype(jnp.bfloat16)
        result = jnp.dot(hidden, down_matrix, preferred_element_type=jnp.float32).astype(jnp.bfloat16)
        weighted = jnp.where(filled, weight_slot, jnp.zeros((), jnp.float32))[:, None] * result.astype(jnp.float32)
        running = running.at[owner_token].add(weighted)
        return (running, None)
    accumulated, unused = lax.scan(one_expert, jnp.zeros((TOKENS, D), jnp.float32), (w_gate, w_up, w_down, jnp.arange(EXPERTS, dtype=jnp.int32)))
    return accumulated.astype(jnp.bfloat16)
```

```python
import functools

import jax
import jax.numpy as jnp
from jax import lax
from jax.experimental import pallas as pl
from jax.experimental.pallas import tpu as pltpu
from jax.sharding import PartitionSpec as P

EPSILON = 1e-06
AXES = ("dp", "expert")
HBM_BUDGET = 112 * 1024 * 1024


def rms_normed(tokens, norm_gain):
    widened = tokens.astype(jnp.float32)
    spread = jnp.mean(widened * widened, axis=-1, keepdims=True)
    return (widened * lax.rsqrt(spread + EPSILON) * norm_gain).astype(jnp.bfloat16)


def expert_kernel(slots, rank_ref, gate_ref, *refs):
    blocks = rank_ref.shape[0]
    xs = refs[:blocks]
    wg_hbm, wu_hbm, wd_hbm, mine_hbm, theirs_hbm = refs[blocks : blocks + 5]
    x_buf, wg, wu, wd, packed, hidden, x_sem, w_sem, out_sem = refs[blocks + 5 :]
    length, width = x_buf.shape[1:]
    inner = wg.shape[1]
    half = blocks // 2
    loads = [
        pltpu.make_async_copy(xs[b], x_buf.at[b], x_sem.at[b]) for b in range(blocks)
    ]
    weight_loads = [
        pltpu.make_async_copy(wg_hbm, wg, w_sem.at[0]),
        pltpu.make_async_copy(wu_hbm, wu, w_sem.at[1]),
        pltpu.make_async_copy(wd_hbm, wd, w_sem.at[2]),
    ]
    for copy in loads + weight_loads:
        copy.start()

    def chooser(b):
        row = rank_ref[pl.ds(b, 1), :]
        return lax.broadcasted_iota(jnp.int32, (slots, length), 0) == row

    cols = 512
    for b in range(blocks):
        loads[b].wait()
        pick = chooser(b).astype(jnp.bfloat16)

        @pl.loop(0, width // cols)
        def _(n, b=b, pick=pick):
            where = pl.ds(pl.multiple_of(n * cols, cols), cols)
            rows = jnp.dot(pick, x_buf[b, :, where], preferred_element_type=jnp.float32)
            packed[pl.ds(b * slots, slots), where] = rows.astype(jnp.bfloat16)

    weight_loads[0].wait()
    weight_loads[1].wait()
    tile = 256

    @pl.loop(0, inner // tile)
    def _(n):
        where = pl.ds(pl.multiple_of(n * tile, tile), tile)
        gate = jnp.dot(packed[...], wg[:, where], preferred_element_type=jnp.float32)
        up = jnp.dot(packed[...], wu[:, where], preferred_element_type=jnp.float32)
        hidden[:, where] = (gate / (1.0 + jnp.exp(-gate)) * up).astype(jnp.bfloat16)

    weight_loads[2].wait()
    picks = [chooser(b) for b in range(blocks)]
    scales = [
        jnp.sum(
            jnp.where(picks[b], gate_ref[pl.ds(b, 1), :], 0.0), axis=1, keepdims=True
        )
        for b in range(blocks)
    ]

    @pl.loop(0, width // tile)
    def _(n):
        where = pl.ds(pl.multiple_of(n * tile, tile), tile)
        result = jnp.dot(hidden[...], wd[:, where], preferred_element_type=jnp.float32)
        for b in range(blocks):
            part = (result[b * slots : (b + 1) * slots] * scales[b]).astype(jnp.bfloat16)
            spread = lax.dot_general(
                picks[b].astype(jnp.bfloat16),
                part,
                (((0,), (0,)), ((), ())),
                preferred_element_type=jnp.float32,
            )
            x_buf[b, :, where] = spread.astype(jnp.bfloat16)

    stores = [
        pltpu.make_async_copy(
            x_buf.at[pl.ds(0, half)], mine_hbm, out_sem.at[0]
        ),
        pltpu.make_async_copy(
            x_buf.at[pl.ds(half, half)], theirs_hbm, out_sem.at[1]
        ),
    ]
    for copy in stores:
        copy.start()
    for copy in stores:
        copy.wait()


def run_expert(slots, rank, gates, xs, w_gate, w_up, w_down):
    blocks = len(xs)
    length, width = xs[0].shape
    inner = w_gate.shape[1]
    rows = blocks * slots
    out = jax.ShapeDtypeStruct((blocks // 2, length, width), jnp.bfloat16)
    anywhere = pl.BlockSpec(memory_space=pl.ANY)
    local = pl.BlockSpec(memory_space=pltpu.VMEM)
    moved = 2 * (2 * blocks * length * width + 3 * width * inner)
    return pl.pallas_call(
        functools.partial(expert_kernel, slots),
        out_shape=(out, out),
        in_specs=[local, local] + [anywhere] * (blocks + 3),
        out_specs=(anywhere, anywhere),
        scratch_shapes=[
            pltpu.VMEM((blocks, length, width), jnp.bfloat16),
            pltpu.VMEM((width, inner), jnp.bfloat16),
            pltpu.VMEM((width, inner), jnp.bfloat16),
            pltpu.VMEM((inner, width), jnp.bfloat16),
            pltpu.VMEM((rows, width), jnp.bfloat16),
            pltpu.VMEM((rows, inner), jnp.bfloat16),
            pltpu.SemaphoreType.DMA((blocks,)),
            pltpu.SemaphoreType.DMA((3,)),
            pltpu.SemaphoreType.DMA((2,)),
        ],
        compiler_params=pltpu.CompilerParams(vmem_limit_bytes=48 * 1024 * 1024),
        cost_estimate=pl.CostEstimate(
            flops=6 * rows * width * inner + 4 * rows * length * width,
            bytes_accessed=moved,
            transcendentals=rows * inner,
        ),
        name="expert",
    )(rank, gates, *xs, w_gate, w_up, w_down)


def tree_body(tokens, norm_gain, recorded_ids, recorded_gates, w_gate, w_up, w_down):
    length, width = tokens.shape
    fan_out = recorded_ids.shape[2]
    dp_count = lax.axis_size("dp")
    expert_count = lax.axis_size("expert")
    experts = dp_count * expert_count
    planes = dp_count // 2
    slots = (3 * length * fan_out + 2 * experts - 1) // (2 * experts)
    capacity = 5 * length * fan_out // 4
    sequences, own_steps = recorded_ids.shape[:2]

    def flat(z, core, y, x):
        return (z % planes * 2 + core) * expert_count + y * 2 + x

    def swaps(target):
        places = [
            (z, c, y, x)
            for z in range(planes)
            for c in range(2)
            for y in range(2)
            for x in range(2)
        ]
        return [(flat(*p), flat(*target(*p))) for p in places]

    first = swaps(lambda z, c, y, x: (z, c, y ^ (c == 0), x ^ (c == 1)))
    second = swaps(lambda z, c, y, x: (z, c, y ^ (c == 1), x ^ (c == 0)))
    partner = swaps(lambda z, c, y, x: (z, 1 - c, y, x))
    onward = swaps(lambda z, c, y, x: (z + 1, c, y, x))

    def send(value, pairs):
        return lax.ppermute(value, AXES, pairs)

    own = rms_normed(tokens, norm_gain)
    held = [own]
    for _ in range(planes - 1):
        held.append(send(held[-1], onward))
    gathered = []
    for block in held:
        near = send(block, first)
        side = send(block, second)
        far = send(near, second)
        group = [block, near, side, far]
        gathered.append(group + [send(piece, partner) for piece in group])

    expert_range = jnp.arange(experts, dtype=jnp.int32)
    named = recorded_ids[None] == expert_range[:, None, None, None]
    spread_gates = jnp.sum(jnp.where(named, recorded_gates[None], 0.0), axis=3)
    routed = lax.all_to_all(
        spread_gates.reshape(experts, sequences * own_steps),
        AXES, split_axis=0, concat_axis=0, tiled=True,
    )
    gates = routed.reshape(experts, sequences, own_steps)
    gates = gates.transpose(1, 0, 2).reshape(sequences, length)
    used = gates > 0.0
    used_half = used.astype(jnp.bfloat16)
    step = jnp.arange(length)
    rank = jnp.dot(
        used_half, (step[:, None] < step[None, :]).astype(jnp.bfloat16),
        preferred_element_type=jnp.float32,
    ).astype(jnp.int32)
    totals = jnp.sum(used.astype(jnp.int32), axis=1)
    seq = jnp.arange(sequences)
    starts = jnp.sum(
        jnp.where(seq[None, :] < seq[:, None], totals[None, :], 0), axis=1
    )
    kept = used & (starts[:, None] + rank < capacity)
    kept_gates = jnp.where(kept, gates, 0.0)
    rank = jnp.where(used, rank, -1)

    dp_at = lax.axis_index("dp")
    at = lax.axis_index("expert")
    z_at, core_at = dp_at // 2, dp_at % 2
    y_at, x_at = at // 2, at % 2
    hops = jnp.arange(planes, dtype=jnp.int32)[:, None, None]
    turned = jnp.arange(2, dtype=jnp.int32)[None, :, None]
    part = jnp.arange(4, dtype=jnp.int32)[None, None, :]
    plane_of = (z_at - hops + planes) % planes
    core_of = core_at ^ turned
    near_or_far = (part == 1) | (part == 3)
    side_or_far = (part == 2) | (part == 3)
    cross_y = jnp.where(core_of == 0, near_or_far, side_or_far).astype(jnp.int32)
    cross_x = jnp.where(core_of == 0, side_or_far, near_or_far).astype(jnp.int32)
    order = (plane_of * 2 + core_of) * expert_count + (y_at ^ cross_y) * 2 + (x_at ^ cross_x)
    order = order.reshape(-1)
    rank = jnp.take(rank, order, axis=0)
    kept_gates = jnp.take(kept_gates, order, axis=0)

    per = 2 * expert_count
    partial_sums = [
        run_expert(
            slots,
            rank[j * per : (j + 1) * per],
            kept_gates[j * per : (j + 1) * per],
            gathered[j],
            w_gate[0], w_up[0], w_down[0],
        )
        for j in range(planes)
    ]

    def added(*terms):
        total = terms[0].astype(jnp.float32)
        for term in terms[1:]:
            total = total + term.astype(jnp.float32)
        return total.astype(jnp.bfloat16)

    carried = None
    for j in [*range(1, planes), 0]:
        mine, theirs = partial_sums[j]
        back = send(theirs, partner)
        far = send(added(mine[3], back[3]), second)
        near = send(added(mine[1], back[1], far), first)
        side = send(added(mine[2], back[2]), second)
        terms = [mine[0], back[0], near, side]
        if carried is not None:
            terms.append(send(carried, onward))
        carried = added(*terms)
    return carried


def body(tokens, norm_gain, recorded_ids, recorded_gates, w_gate, w_up, w_down):
    normed = rms_normed(tokens, norm_gain)
    length = tokens.shape[0]
    model_width = tokens.shape[1]
    fan_out = recorded_ids.shape[2]
    dp_count = lax.axis_size("dp")
    expert_count = lax.axis_size("expert")
    experts = dp_count * expert_count
    pair_slots = (3 * length * fan_out + 2 * experts - 1) // (2 * experts)
    capacity = 5 * length * fan_out // 4
    id_values = recorded_ids.astype(jnp.float32)
    expert_range = jnp.arange(experts, dtype=jnp.int32)
    seq_ids, seq_gates = (
        lax.all_to_all(id_values, ("dp", "expert"), split_axis=0, concat_axis=1, tiled=True),
        lax.all_to_all(recorded_gates, ("dp", "expert"), split_axis=0, concat_axis=1, tiled=True),
    )
    route_ids = seq_ids.astype(jnp.int32).reshape(-1)
    route_gates = seq_gates.reshape(-1)
    onehot = (route_ids[:, None] == expert_range[None, :]).astype(jnp.bfloat16)
    own_counts = jnp.sum(onehot.astype(jnp.float32), axis=0).astype(jnp.int32)
    source_loads = lax.all_to_all(
        own_counts, ("dp", "expert"), split_axis=0, concat_axis=0, tiled=True
    )
    assignments = length * fan_out
    order_index = jnp.arange(assignments, dtype=jnp.int32)
    earlier_mask = (order_index[:, None] > order_index[None, :]).astype(jnp.bfloat16)
    before = jnp.dot(earlier_mask, onehot, preferred_element_type=jnp.float32)
    queue_rank = jnp.sum(before * onehot.astype(jnp.float32), axis=1).astype(jnp.int32)
    slot_row = route_ids * pair_slots + queue_rank
    slot_range = jnp.arange(experts * pair_slots, dtype=jnp.int32)
    dispatch_map = jnp.any(
        slot_range[:, None, None] == slot_row.reshape(length, fan_out)[None, :, :], axis=2
    )
    outgoing = jnp.dot(
        dispatch_map.astype(jnp.bfloat16), normed, preferred_element_type=jnp.float32
    )
    outgoing = outgoing.astype(jnp.bfloat16).reshape(experts, pair_slots, model_width)
    arrived = lax.all_to_all(outgoing, ("dp", "expert"), split_axis=0, concat_axis=0, tiled=True)
    starts = jnp.cumsum(source_loads) - source_loads
    queue_ends = starts + source_loads
    queue_total = queue_ends[experts - 1]
    places = jnp.arange(capacity, dtype=jnp.int32)
    source = jnp.sum((queue_ends[None, :] <= places[:, None]).astype(jnp.int32), axis=1)
    occupied = places < queue_total
    src_clip = jnp.minimum(source, experts - 1)
    offset_in = jnp.clip(places - starts[src_clip], 0, pair_slots - 1)
    row_index = src_clip * pair_slots + offset_in
    arrived_rows = arrived.reshape(experts * pair_slots, model_width)
    packed = jnp.where(
        occupied[:, None], jnp.take(arrived_rows, row_index, axis=0), jnp.zeros((), jnp.bfloat16)
    )
    gate_part = jnp.dot(packed, w_gate[0], preferred_element_type=jnp.float32)
    up_part = jnp.dot(packed, w_up[0], preferred_element_type=jnp.float32)
    hidden = (jax.nn.silu(gate_part) * up_part).astype(jnp.bfloat16)
    result = jnp.dot(hidden, w_down[0], preferred_element_type=jnp.float32).astype(jnp.bfloat16)
    slot_index = jnp.arange(pair_slots, dtype=jnp.int32)
    target_place = starts[:, None] + slot_index[None, :]
    slot_valid = (slot_index[None, :] < source_loads[:, None]) & (target_place < capacity)
    fetched = jnp.take(result, jnp.clip(target_place, 0, capacity - 1).reshape(-1), axis=0)
    returning = jnp.where(slot_valid.reshape(-1)[:, None], fetched, jnp.zeros((), jnp.bfloat16))
    returning = returning.reshape(experts, pair_slots, model_width)
    answered = lax.all_to_all(returning, ("dp", "expert"), split_axis=0, concat_axis=0, tiled=True)
    answered_rows = answered.reshape(experts * pair_slots, model_width)
    picked = jnp.take(answered_rows, slot_row, axis=0).astype(jnp.float32)
    weighted = (picked * route_gates[:, None]).reshape(length, fan_out, model_width)
    combined = jnp.sum(weighted, axis=1)
    return combined.astype(jnp.bfloat16)


def solution(mesh):
    dp_count, expert_count = mesh.shape["dp"], mesh.shape["expert"]

    def chosen(tokens, *rest):
        everywhere = 2 * 2 * dp_count * expert_count * tokens.shape[0] * tokens.shape[1]
        in_pairs = dp_count % 2 == 0 and expert_count == 2 * 2
        plan = tree_body if in_pairs and everywhere <= HBM_BUDGET else body
        return plan(tokens, *rest)

    in_specs = (
        P(("dp", "expert"), None),
        P(),
        P(None, ("dp", "expert"), None),
        P(None, ("dp", "expert"), None),
        P(("dp", "expert"), None, None),
        P(("dp", "expert"), None, None),
        P(("dp", "expert"), None, None),
    )
    out_specs = P(("dp", "expert"), None)
    return jax.shard_map(chosen, mesh=mesh, in_specs=in_specs, out_specs=out_specs, check_vma=False)
```
